256 devices in a mesh: row: 16 (over y, z_hi, core), col: 16 (over z_lo, x).
Axes of the slice: x: 4, y: 4, z: 8 (z_hi: 2, z_lo: 4; z = z_hi * 4 + z_lo), core: 2. Of those that a mesh axis runs over, the one named last changes fastest.
Arguments:
- fluid_data: float32 [51, 32768], P(None, ('row', 'col')), as said below
- center_data: float32 [51, 16384], P(None, ('col', 'row')), as said below
- poly_coef: float32 [48, 4], replicated, may hold values from -3 to 3
Outputs:
- fluid_motion: float32 [48, 32768], P(None, ('row', 'col'))
- center_load: float32 [48, 16384], P(None, ('col', 'row'))
The draws below stay inside these ranges and needn't reach their ends.
Inputs may be any that keep to these rules, and one draw needn't show every extreme that they name: Rows 0 to 2 of fluid_data lie in [0, 1]; rows 3 and on are forces. Rows 0 and 1 of center_data lie in [0, 1] and row 2 lies in [-0.5, -0.02], so every center is at least 0.02 below every vertex; rows 3 and on are coefficients.
All inputs are finite; a program needn't handle non-finite values.
Results may differ from the reference program's by a relative error of at most 0.0003.
Values sent between devices are 32-bit elements; how exact they have to be, the bound alone decides.
No kernel may reach another device: no remote copies, remote signals or barrier semaphores. Data moves between devices by JAX's collectives and lax.ppermute only.
A program may use at most 64 MiB of HBM per device.

```python
import math
import jax
import jax.numpy as jnp
from jax import lax

WAVES = 64
COLS = 48
FLUID = 32768
CENTERS = 16384


def draw_fluid_data(key, part):
    first, second = jax.random.split(jax.random.fold_in(key, 11))
    places = jax.random.uniform(first, (3, FLUID), jnp.float32)
    spread = 2.0 * math.pi * WAVES * math.sqrt(0.8 / FLUID)
    values = jax.random.normal(second, (COLS, FLUID), jnp.float32) * spread
    return jnp.concatenate([places, values], axis=0)


def draw_center_data(key, part):
    first, second, third = jax.random.split(jax.random.fold_in(key, 23), 3)
    plane = jax.random.uniform(first, (2, CENTERS), jnp.float32)
    depth = jax.random.uniform(second, (1, CENTERS), jnp.float32)
    spread = 2.0 * math.pi * WAVES * math.sqrt(0.8 / CENTERS)
    height = -0.02 - 0.48 * depth
    values = jax.random.normal(third, (COLS, CENTERS), jnp.float32) * spread
    return jnp.concatenate([plane, height, values], axis=0)


def noise(key, dims, scale, limit, kind=jnp.bfloat16):
    entries = scale * jax.random.normal(key, dims, jnp.float32)
    return jnp.clip(entries, min=-limit, max=limit).astype(kind)


def setup_inputs(seed: int = 0) -> dict:
    streams_of = jax.random.split(jax.random.key(seed), 4)
    fluid_data = draw_fluid_data(jax.random.fold_in(streams_of[3], 71), 0)
    center_data = draw_center_data(jax.random.fold_in(streams_of[3], 71), 0)
    poly_coef = noise(streams_of[2], (COLS, 4), 0.5, 3.0, jnp.float32)
    return dict(fluid_data=fluid_data, center_data=center_data, poly_coef=poly_coef)


def kernel_block(center_pos, fluid_pos):
    dx = center_pos[0][:, None] - fluid_pos[0][None, :]
    dy = center_pos[1][:, None] - fluid_pos[1][None, :]
    dz = center_pos[2][:, None] - fluid_pos[2][None, :]
    sq = dx * dx + dy * dy + dz * dz
    phase = 2.0 * math.pi * WAVES * jnp.sqrt(sq)
    return jnp.sin(phase) / phase

def reference(fluid_data, center_data, poly_coef):
    total = center_data.shape[1]
    width = fluid_data.shape[1]
    block = math.gcd(total, 256)
    count = total // block
    fluid_pos = fluid_data[:3]
    forces = fluid_data[3:]
    pieces = center_data.reshape(center_data.shape[0], count, block).transpose(1, 0, 2)

    def step(motion, piece):
        tile = kernel_block(piece[:3], fluid_pos)
        motion = motion + jnp.dot(piece[3:], tile, precision=lax.Precision.HIGHEST, preferred_element_type=jnp.float32)
        back = lax.dot_general(forces, tile, (((1,), (1,)), ((), ())), precision=lax.Precision.HIGHEST, preferred_element_type=jnp.float32)
        return (motion, back)
    start = jnp.zeros((forces.shape[0], width), jnp.float32)
    motion, backs = lax.scan(step, start, pieces)
    loads = backs.transpose(1, 0, 2).reshape(forces.shape[0], total)
    affine = poly_coef[:, 0:1] + jnp.dot(poly_coef[:, 1:], fluid_pos, precision=lax.Precision.HIGHEST, preferred_element_type=jnp.float32)
    return (motion + affine, loads)
```

```python
import jax
import jax.numpy as jnp
from jax import lax
from jax.experimental import pallas as pl
from jax.experimental.pallas import tpu as pltpu
from jax.sharding import PartitionSpec as P

WAVES = 64
COLS = 48
LANES = 128
LEAD = -1.9530316595457846
TAIL = (-3.3578779781881196, 6.240606194702548, -6.649373004251278, 3.3689630874951395, -0.5120242670059871)

def tile_values(cx, cy, cz, fx, fy, fz):
    dx = cx - fx
    dy = cy - fy
    dz = cz - fz
    sq = dx * dx + dy * dy + dz * dz
    inv = lax.rsqrt(sq)
    turns = sq * inv
    rest = turns - jnp.round(turns)
    z = rest * rest
    p = z + TAIL[0]
    for c in TAIL[1:]:
        p = p * z + c
    return (rest * inv) * p

def split(a):
    hi = a.astype(jnp.bfloat16)
    lo = (a - hi.astype(jnp.float32)).astype(jnp.bfloat16)
    return hi, lo

def coupling_body(fluid, center, motion_out, load_out, cpos, cval, fval, fpos, t0, t1, acc, loads):
    nf = fluid.shape[0]
    nb = center.shape[0] // 2
    width = nf * LANES
    half = lax.broadcasted_iota(jnp.int32, (1, LANES), 1) < LANES // 2
    for k in range(nf):
        hi, lo = split(fluid[k, 0:COLS, :] * LEAD)
        fval[0:COLS, k * LANES:(k + 1) * LANES] = hi
        fval[COLS:2 * COLS, k * LANES:(k + 1) * LANES] = lo
        fpos[:, k * LANES:(k + 1) * LANES] = fluid[k, COLS:COLS + 3, :] * float(WAVES)
    for b in range(nb):
        one = center[2 * b]
        two = center[2 * b + 1]
        top = jnp.where(half, one, pltpu.roll(two, LANES // 2, 1))
        bot = jnp.where(half, pltpu.roll(one, LANES // 2, 1), two)
        val = jnp.concatenate([top[0:24], bot[0:24]], 0) * LEAD
        hi, lo = split(val)
        v = jnp.concatenate([hi, lo], 0)
        cval[b, :, 0:LANES] = v
        cval[b, :, LANES:2 * LANES] = v
        pos = jnp.concatenate([top[24:26], bot[24:25], jnp.zeros((5, LANES), jnp.float32)], 0) * float(WAVES)
        post = jnp.transpose(pos)
        for a in range(3):
            cpos[a, b * LANES:(b + 1) * LANES, :] = jnp.broadcast_to(post[:, a:a + 1], (LANES, LANES))

    acc[...] = jnp.zeros_like(acc)

    def compute(b, t):
        for k in range(nf):
            s = pl.ds(k * LANES, LANES)
            fx = fpos[0:1, s]; fy = fpos[1:2, s]; fz = fpos[2:3, s]
            for g in range(LANES // 16):
                rows = pl.ds(b * LANES + g * 16, 16)
                v = tile_values(cpos[0, rows, :], cpos[1, rows, :], cpos[2, rows, :], fx, fy, fz)
                hi, lo = split(v)
                t[g * 16:(g + 1) * 16, s] = hi
                t[LANES + g * 16:LANES + (g + 1) * 16, s] = lo

    def dots(b, t):
        acc[...] += jnp.dot(cval[b], t[...], preferred_element_type=jnp.float32)
        back = lax.dot_general(t[...], fval[...], (((1,), (1,)), ((), ())), preferred_element_type=jnp.float32)
        loads[pl.ds(b * LANES, LANES), :] = back[0:LANES, :] + back[LANES:2 * LANES, :]

    compute(0, t0)
    def pair(p, c):
        compute(2 * p + 1, t1)
        dots(2 * p, t0)
        compute(2 * p + 2, t0)
        dots(2 * p + 1, t1)
        return c
    lax.fori_loop(0, nb // 2 - 1, pair, 0)
    compute(nb - 1, t1)
    dots(nb - 2, t0)
    dots(nb - 1, t1)

    for k in range(nf):
        s = slice(k * LANES, (k + 1) * LANES)
        motion_out[k] = acc[0:COLS, s] + acc[COLS:2 * COLS, s]
    for b in range(nb):
        l = jnp.transpose(loads[b * LANES:(b + 1) * LANES, :])
        l = l[0:COLS] + l[COLS:2 * COLS]
        top = l[0:24]
        bot = l[24:48]
        load_out[2 * b] = jnp.where(half, top, pltpu.roll(bot, LANES // 2, 1))
        load_out[2 * b + 1] = jnp.where(half, pltpu.roll(top, LANES // 2, 1), bot)

def coupling(fluid, center):
    nf = fluid.shape[0]
    nc = center.shape[0]
    nb = nc // 2
    width = nf * LANES
    return pl.pallas_call(
        coupling_body,
        out_shape=(jax.ShapeDtypeStruct((nf, COLS, LANES), jnp.float32), jax.ShapeDtypeStruct((nc, 24, LANES), jnp.float32)),
        in_specs=[pl.BlockSpec(memory_space=pltpu.VMEM)] * 2,
        out_specs=(pl.BlockSpec(memory_space=pltpu.VMEM),) * 2,
        scratch_shapes=[
            pltpu.VMEM((3, nb * LANES, LANES), jnp.float32),
            pltpu.VMEM((nb, 2 * COLS, 2 * LANES), jnp.bfloat16),
            pltpu.VMEM((2 * COLS, width), jnp.bfloat16),
            pltpu.VMEM((3, width), jnp.float32),
            pltpu.VMEM((2 * LANES, width), jnp.bfloat16),
            pltpu.VMEM((2 * LANES, width), jnp.bfloat16),
            pltpu.VMEM((2 * COLS, width), jnp.float32),
            pltpu.VMEM((nb * LANES, 2 * COLS), jnp.float32),
        ],
        name="coupling",
    )(fluid, center)


def from_everyone(array, axis):
    devices = lax.axis_size(axis)
    return lax.all_to_all(jnp.broadcast_to(array[None], (devices, *array.shape)), axis, 0, 0, tiled=True)


def sum_at_owner(parts, axis):
    return lax.all_to_all(parts, axis, 0, 0, tiled=True).sum(axis=0)


def per_device(fluid_data, center_data, poly_coef):
    fluid = jnp.concatenate([fluid_data[3:], fluid_data[:3]], 0)
    places = jnp.concatenate([center_data[0:2], center_data[2:3], jnp.zeros_like(center_data[:1])], 0)
    center = jnp.concatenate(
        [
            jnp.concatenate([center_data[3:27], center_data[27:51]], 1),
            jnp.concatenate([places[0:2], places[2:4]], 1),
        ],
        0,
    )
    partial_motion, partial_loads = coupling(from_everyone(fluid, "col"), from_everyone(center, "row"))
    loads = sum_at_owner(partial_loads, "row")
    motion = sum_at_owner(partial_motion, "col")
    affine = poly_coef[:, 0:1] + jnp.dot(
        poly_coef[:, 1:],
        fluid_data[:3],
        precision=lax.Precision.HIGHEST,
        preferred_element_type=jnp.float32,
    )
    half = center_data.shape[1]
    return (motion + affine, jnp.concatenate([loads[:, :half], loads[:, half:]], 0))


def solution(mesh):
    placed = (P(None, ("row", "col")), P(None, ("col", "row")), P())
    return jax.shard_map(
        per_device,
        mesh=mesh,
        in_specs=placed,
        out_specs=(P(None, ("row", "col")), P(None, ("col", "row"))),
        check_vma=False,
    )
```

```python
import jax
import jax.numpy as jnp
from jax import lax
from jax.experimental import pallas as pl
from jax.experimental.pallas import tpu as pltpu
from jax.sharding import PartitionSpec as P

WAVES = 64
COLS = 48
LANES = 128
LEAD = -1.9530316595457846
TAIL = (-3.3578779781881196, 6.240606194702548, -6.649373004251278, 3.3689630874951395, -0.5120242670059871)

def tile_values(cx, cy, cz, fx, fy, fz):
    dx = cx - fx
    dy = cy - fy
    dz = cz - fz
    sq = dx * dx + dy * dy + dz * dz
    inv = lax.rsqrt(sq)
    turns = sq * inv
    rest = turns - jnp.round(turns)
    z = rest * rest
    p = z + TAIL[0]
    for c in TAIL[1:]:
        p = p * z + c
    return (rest * inv) * p

def split(a):
    hi = a.astype(jnp.bfloat16)
    lo = (a - hi.astype(jnp.float32)).astype(jnp.bfloat16)
    return hi, lo

def coupling_body(fluid_a, fluid_b, center_a, center_b, motion_a, motion_b, load_a, load_b, cpos, cval, fval, fpos, t0, t1, acc, loads):
    hf = fluid_a.shape[0]
    nf = 2 * hf
    hb = center_a.shape[0] // 2
    nb = 2 * hb
    width = nf * LANES
    half = lax.broadcasted_iota(jnp.int32, (1, LANES), 1) < LANES // 2
    for k in range(nf):
        chunk = (fluid_a, fluid_b)[k // hf].at[k % hf]
        hi, lo = split(chunk[0:COLS, :] * LEAD)
        fval[0:COLS, k * LANES:(k + 1) * LANES] = hi
        fval[COLS:2 * COLS, k * LANES:(k + 1) * LANES] = lo
        fpos[:, k * LANES:(k + 1) * LANES] = chunk[COLS:COLS + 3, :] * float(WAVES)
    for b in range(nb):
        side = (center_a, center_b)[b // hb]
        one = side[2 * (b % hb)]
        two = side[2 * (b % hb) + 1]
        top = jnp.where(half, one, pltpu.roll(two, LANES // 2, 1))
        bot = jnp.where(half, pltpu.roll(one, LANES // 2, 1), two)
        val = jnp.concatenate([top[0:24], bot[0:24]], 0) * LEAD
        hi, lo = split(val)
        v = jnp.concatenate([hi, lo], 0)
        cval[b, :, 0:LANES] = v
        cval[b, :, LANES:2 * LANES] = v
        pos = jnp.concatenate([top[24:26], bot[24:25], jnp.zeros((5, LANES), jnp.float32)], 0) * float(WAVES)
        post = jnp.transpose(pos)
        for a in range(3):
            cpos[a, b * LANES:(b + 1) * LANES, :] = jnp.broadcast_to(post[:, a:a + 1], (LANES, LANES))

    acc[...] = jnp.zeros_like(acc)

    def compute(b, t):
        for k in range(nf):
            s = pl.ds(k * LANES, LANES)
            fx = fpos[0:1, s]; fy = fpos[1:2, s]; fz = fpos[2:3, s]
            for g in range(LANES // 16):
                rows = pl.ds(b * LANES + g * 16, 16)
                v = tile_values(cpos[0, rows, :], cpos[1, rows, :], cpos[2, rows, :], fx, fy, fz)
                hi, lo = split(v)
                t[g * 16:(g + 1) * 16, s] = hi
                t[LANES + g * 16:LANES + (g + 1) * 16, s] = lo

    def dots(b, t):
        acc[...] += jnp.dot(cval[b], t[...], preferred_element_type=jnp.float32)
        back = lax.dot_general(t[...], fval[...], (((1,), (1,)), ((), ())), preferred_element_type=jnp.float32)
        loads[pl.ds(b * LANES, LANES), :] = back[0:LANES, :] + back[LANES:2 * LANES, :]

    compute(0, t0)
    def pair(p, c):
        compute(2 * p + 1, t1)
        dots(2 * p, t0)
        compute(2 * p + 2, t0)
        dots(2 * p + 1, t1)
        return c
    lax.fori_loop(0, nb // 2 - 1, pair, 0)
    compute(nb - 1, t1)
    dots(nb - 2, t0)
    dots(nb - 1, t1)

    for k in range(nf):
        s = slice(k * LANES, (k + 1) * LANES)
        (motion_a, motion_b)[k // hf][k % hf] = acc[0:COLS, s] + acc[COLS:2 * COLS, s]
    for b in range(nb):
        l = jnp.transpose(loads[b * LANES:(b + 1) * LANES, :])
        l = l[0:COLS] + l[COLS:2 * COLS]
        top = l[0:24]
        bot = l[24:48]
        side = (load_a, load_b)[b // hb]
        side[2 * (b % hb)] = jnp.where(half, top, pltpu.roll(bot, LANES // 2, 1))
        side[2 * (b % hb) + 1] = jnp.where(half, pltpu.roll(top, LANES // 2, 1), bot)

def coupling(fluid_a, fluid_b, center_a, center_b):
    hf = fluid_a.shape[0]
    hc = center_a.shape[0]
    nb = hc
    width = 2 * hf * LANES
    motion = jax.ShapeDtypeStruct((hf, COLS, LANES), jnp.float32)
    load = jax.ShapeDtypeStruct((hc, COLS // 2, LANES), jnp.float32)
    return pl.pallas_call(
        coupling_body,
        out_shape=(motion, motion, load, load),
        in_specs=[pl.BlockSpec(memory_space=pltpu.VMEM)] * 4,
        out_specs=(pl.BlockSpec(memory_space=pltpu.VMEM),) * 4,
        scratch_shapes=[
            pltpu.VMEM((3, nb * LANES, LANES), jnp.float32),
            pltpu.VMEM((nb, 2 * COLS, 2 * LANES), jnp.bfloat16),
            pltpu.VMEM((2 * COLS, width), jnp.bfloat16),
            pltpu.VMEM((3, width), jnp.float32),
            pltpu.VMEM((2 * LANES, width), jnp.bfloat16),
            pltpu.VMEM((2 * LANES, width), jnp.bfloat16),
            pltpu.VMEM((2 * COLS, width), jnp.float32),
            pltpu.VMEM((nb * LANES, 2 * COLS), jnp.float32),
        ],
        name="coupling",
    )(fluid_a, fluid_b, center_a, center_b)


AXES = ("row", "col")


def place(x, y, z, core):
    return (y * 4 + (z // 4) * 2 + core) * 16 + (z % 4) * 4 + x


def partners(move):
    spots = [(x, y, z, c) for x in range(4) for y in range(4) for z in range(8) for c in range(2)]
    return [(place(*spot), place(*move(*spot))) for spot in spots]


def near(v):
    return v ^ 1


def wrap(v):
    return 3 - v


FLUID_STAGES = (
    partners(lambda x, y, z, c: (near(x), y, z, c)),
    partners(lambda x, y, z, c: (wrap(x), y, z, c)),
    partners(lambda x, y, z, c: (x, y, z ^ 1, c)),
    partners(lambda x, y, z, c: (x, y, z, 1 - c)),
)
CENTER_STAGES = (
    partners(lambda x, y, z, c: (x, y, 2 * near(z // 2) + z % 2, c)),
    partners(lambda x, y, z, c: (x, y, 2 * wrap(z // 2) + z % 2, c)),
    partners(lambda x, y, z, c: (x, near(y), z, c)),
    partners(lambda x, y, z, c: (x, wrap(y), z, c)),
)


def gather_step(held, stage):
    return held, lax.ppermute(held, AXES, stage)


def sum_step(mine, theirs, stage):
    arrived = lax.ppermute(theirs, AXES, stage)
    half = mine.shape[0] // 2
    return mine[:half] + arrived[:half], mine[half:] + arrived[half:]


def per_device(fluid_data, center_data, poly_coef):
    fluid = jnp.concatenate([fluid_data[3:], fluid_data[:3]], 0)
    places = jnp.concatenate([center_data[0:2], center_data[2:3], jnp.zeros_like(center_data[:1])], 0)
    center = jnp.concatenate(
        [
            jnp.concatenate([center_data[3:27], center_data[27:51]], 1),
            jnp.concatenate([places[0:2], places[2:4]], 1),
        ],
        0,
    )
    fluid = fluid[None]
    center = center[None]
    fluids = (fluid, None)
    centers = (center, None)
    for i in range(4):
        held = fluids[0] if i == 0 else jnp.concatenate(fluids, 0)
        fluids = gather_step(held, FLUID_STAGES[i])
        held = centers[0] if i == 0 else jnp.concatenate(centers, 0)
        centers = gather_step(held, CENTER_STAGES[i])
    motion, motion_away, loads, loads_away = coupling(*fluids, *centers)
    for i in (3, 2, 1):
        motion, motion_away = sum_step(motion, motion_away, FLUID_STAGES[i])
        loads, loads_away = sum_step(loads, loads_away, CENTER_STAGES[i])
    motion = (motion + lax.ppermute(motion_away, AXES, FLUID_STAGES[0]))[0]
    loads = (loads + lax.ppermute(loads_away, AXES, CENTER_STAGES[0]))[0]
    affine = poly_coef[:, 0:1] + jnp.dot(
        poly_coef[:, 1:],
        fluid_data[:3],
        precision=lax.Precision.HIGHEST,
        preferred_element_type=jnp.float32,
    )
    half = center_data.shape[1]
    return (motion + affine, jnp.concatenate([loads[:, :half], loads[:, half:]], 0))


def solution(mesh):
    placed = (P(None, ("row", "col")), P(None, ("col", "row")), P())
    return jax.shard_map(
        per_device,
        mesh=mesh,
        in_specs=placed,
        out_specs=(P(None, ("row", "col")), P(None, ("col", "row"))),
        check_vma=False,
    )
```

```python
import jax
import jax.numpy as jnp
from jax import lax
from jax.experimental import pallas as pl
from jax.experimental.pallas import tpu as pltpu
from jax.sharding import PartitionSpec as P


WAVES = 64
COLS = 48
LANES = 128
LEAD = -1.9530316595457846
TAIL = (-3.3578779781881196, 6.240606194702548, -6.649373004251278, 3.3689630874951395, -0.5120242670059871)


def tile_values(cx, cy, cz, fx, fy, fz):
    dx = cx - fx
    dy = cy - fy
    dz = cz - fz
    sq = dx * dx + dy * dy + dz * dz
    inv = lax.rsqrt(sq)
    turns = sq * inv
    rest = turns - jnp.round(turns)
    z = rest * rest
    p = z + TAIL[0]
    for c in TAIL[1:]:
        p = p * z + c
    return (rest * inv) * p


def split(a):
    hi = a.astype(jnp.bfloat16)
    lo = (a - hi.astype(jnp.float32)).astype(jnp.bfloat16)
    return hi, lo


def coupling_body(fluid_a, fluid_b, center_a, center_b, motion_a, motion_b, load_a, load_b, cpos, cval, fval, fpos, t0, t1, acc, loads):
    hf = fluid_a.shape[0]
    nf = 2 * hf
    hb = center_a.shape[0] // 2
    nb = 2 * hb
    half = lax.broadcasted_iota(jnp.int32, (1, LANES), 1) < LANES // 2
    for k in range(nf):
        chunk = (fluid_a, fluid_b)[k // hf].at[k % hf]
        hi, lo = split(chunk[3:3 + COLS, :] * LEAD)
        fval[0:COLS, k * LANES:(k + 1) * LANES] = hi
        fval[COLS:2 * COLS, k * LANES:(k + 1) * LANES] = lo
        fpos[:, k * LANES:(k + 1) * LANES] = chunk[0:3, :] * float(WAVES)
    for b in range(nb):
        side = (center_a, center_b)[b // hb]
        one = side[2 * (b % hb)]
        two = side[2 * (b % hb) + 1]
        top = jnp.where(half, one, pltpu.roll(two, LANES // 2, 1))
        bot = jnp.where(half, pltpu.roll(one, LANES // 2, 1), two)
        val = jnp.concatenate([top[0:24], bot[0:24]], 0) * LEAD
        hi, lo = split(val)
        v = jnp.concatenate([hi, lo], 0)
        cval[b, :, 0:LANES] = v
        cval[b, :, LANES:2 * LANES] = v
        pos = jnp.concatenate([top[24:26], bot[24:25], jnp.zeros((5, LANES), jnp.float32)], 0) * float(WAVES)
        post = jnp.transpose(pos)
        for a in range(3):
            cpos[a, b * LANES:(b + 1) * LANES, :] = jnp.broadcast_to(post[:, a:a + 1], (LANES, LANES))

    acc[...] = jnp.zeros_like(acc)

    def compute(b, t):
        for k in range(nf):
            s = pl.ds(k * LANES, LANES)
            fx = fpos[0:1, s]; fy = fpos[1:2, s]; fz = fpos[2:3, s]
            for g in range(LANES // 16):
                rows = pl.ds(b * LANES + g * 16, 16)
                v = tile_values(cpos[0, rows, :], cpos[1, rows, :], cpos[2, rows, :], fx, fy, fz)
                hi, lo = split(v)
                t[g * 16:(g + 1) * 16, s] = hi
                t[LANES + g * 16:LANES + (g + 1) * 16, s] = lo

    def dots(b, t):
        acc[...] += jnp.dot(cval[b], t[...], preferred_element_type=jnp.float32)
        back = lax.dot_general(t[...], fval[...], (((1,), (1,)), ((), ())), preferred_element_type=jnp.float32)
        loads[pl.ds(b * LANES, LANES), :] = back[0:LANES, :] + back[LANES:2 * LANES, :]

    compute(0, t0)

    def pair(p, c):
        compute(2 * p + 1, t1)
        dots(2 * p, t0)
        compute(2 * p + 2, t0)
        dots(2 * p + 1, t1)
        return c

    lax.fori_loop(0, nb // 2 - 1, pair, 0)
    compute(nb - 1, t1)
    dots(nb - 2, t0)
    dots(nb - 1, t1)

    for k in range(nf):
        s = slice(k * LANES, (k + 1) * LANES)
        (motion_a, motion_b)[k // hf][k % hf] = acc[0:COLS, s] + acc[COLS:2 * COLS, s]
    for b in range(nb):
        l = jnp.transpose(loads[b * LANES:(b + 1) * LANES, :])
        l = l[0:COLS] + l[COLS:2 * COLS]
        top = l[0:24]
        bot = l[24:48]
        side = (load_a, load_b)[b // hb]
        side[2 * (b % hb)] = jnp.where(half, top, pltpu.roll(bot, LANES // 2, 1))
        side[2 * (b % hb) + 1] = jnp.where(half, pltpu.roll(top, LANES // 2, 1), bot)


def coupling(fluid_a, fluid_b, center_a, center_b):
    hf = fluid_a.shape[0]
    hc = center_a.shape[0]
    nb = hc
    width = 2 * hf * LANES
    motion = jax.ShapeDtypeStruct((hf, COLS, LANES), jnp.float32)
    load = jax.ShapeDtypeStruct((hc, COLS // 2, LANES), jnp.float32)
    return pl.pallas_call(
        coupling_body,
        out_shape=(motion, motion, load, load),
        in_specs=[pl.BlockSpec(memory_space=pltpu.VMEM)] * 4,
        out_specs=(pl.BlockSpec(memory_space=pltpu.VMEM),) * 4,
        scratch_shapes=[
            pltpu.VMEM((3, nb * LANES, LANES), jnp.float32),
            pltpu.VMEM((nb, 2 * COLS, 2 * LANES), jnp.bfloat16),
            pltpu.VMEM((2 * COLS, width), jnp.bfloat16),
            pltpu.VMEM((3, width), jnp.float32),
            pltpu.VMEM((2 * LANES, width), jnp.bfloat16),
            pltpu.VMEM((2 * LANES, width), jnp.bfloat16),
            pltpu.VMEM((2 * COLS, width), jnp.float32),
            pltpu.VMEM((nb * LANES, 2 * COLS), jnp.float32),
        ],
        compiler_params=pltpu.CompilerParams(vmem_limit_bytes=16 * 2**20),
        name="coupling",
    )(fluid_a, fluid_b, center_a, center_b)


def pack_body(center, out):
    half = center.shape[1]
    out[0:24, 0:half] = center[3:27, :]
    out[0:24, half:] = center[27:51, :]
    out[24:26, 0:half] = center[0:2, :]
    out[24:25, half:] = center[2:3, :]
    out[25:26, half:] = jnp.zeros((1, half), jnp.float32)


def packed(center):
    return pl.pallas_call(
        pack_body,
        out_shape=jax.ShapeDtypeStruct((26, LANES), jnp.float32),
        in_specs=[pl.BlockSpec(memory_space=pltpu.VMEM)],
        out_specs=pl.BlockSpec(memory_space=pltpu.VMEM),
        compiler_params=pltpu.CompilerParams(vmem_limit_bytes=2**20),
        name="pack",
    )(center)


AXES = ("row", "col")


def place(x, y, z, core):
    return (y * 4 + (z // 4) * 2 + core) * 16 + (z % 4) * 4 + x


def partners(move):
    spots = [(x, y, z, c) for x in range(4) for y in range(4) for z in range(8) for c in range(2)]
    return [(place(*spot), place(*move(*spot))) for spot in spots]


def near(v):
    return v ^ 1


def wrap(v):
    return 3 - v


FLUID_STAGES = (
    partners(lambda x, y, z, c: (near(x), y, z, c)),
    partners(lambda x, y, z, c: (wrap(x), y, z, c)),
    partners(lambda x, y, z, c: (x, y, z ^ 1, c)),
    partners(lambda x, y, z, c: (x, y, z, 1 - c)),
)
CENTER_STAGES = (
    partners(lambda x, y, z, c: (x, y, 2 * near(z // 2) + z % 2, c)),
    partners(lambda x, y, z, c: (x, y, 2 * wrap(z // 2) + z % 2, c)),
    partners(lambda x, y, z, c: (x, near(y), z, c)),
    partners(lambda x, y, z, c: (x, wrap(y), z, c)),
)


def gather_step(held, stage):
    return held, lax.ppermute(held, AXES, stage)


def sum_step(mine, theirs, stage):
    arrived = lax.ppermute(theirs, AXES, stage)
    half = mine.shape[0] // 2
    return mine[:half] + arrived[:half], mine[half:] + arrived[half:]


def per_device(fluid_data, center_data, poly_coef):
    fluid = fluid_data[None]
    center = packed(center_data)[None]
    fluids = (fluid, None)
    centers = (center, None)
    for i in range(4):
        held = fluids[0] if i == 0 else jnp.concatenate(fluids, 0)
        fluids = gather_step(held, FLUID_STAGES[i])
        held = centers[0] if i == 0 else jnp.concatenate(centers, 0)
        centers = gather_step(held, CENTER_STAGES[i])
    motion, motion_away, loads, loads_away = coupling(*fluids, *centers)
    for i in (3, 2, 1):
        loads, loads_away = sum_step(loads, loads_away, CENTER_STAGES[i])
        motion, motion_away = sum_step(motion, motion_away, FLUID_STAGES[i])
    loads = (loads + lax.ppermute(loads_away, AXES, CENTER_STAGES[0]))[0]
    motion = (motion + lax.ppermute(motion_away, AXES, FLUID_STAGES[0]))[0]
    affine = poly_coef[:, 0:1] + jnp.dot(
        poly_coef[:, 1:],
        fluid_data[:3],
        precision=lax.Precision.HIGHEST,
        preferred_element_type=jnp.float32,
    )
    half = center_data.shape[1]
    return (motion + affine, jnp.concatenate([loads[:, :half], loads[:, half:]], 0))


def solution(mesh):
    placed = (P(None, ("row", "col")), P(None, ("col", "row")), P())
    return jax.shard_map(
        per_device,
        mesh=mesh,
        in_specs=placed,
        out_specs=(P(None, ("row", "col")), P(None, ("col", "row"))),
        check_vma=False,
    )
```

```python
import jax
import jax.numpy as jnp
from jax import lax
from jax.experimental import pallas as pl
from jax.experimental.pallas import tpu as pltpu
from jax.sharding import PartitionSpec as P


WAVES = 64
COLS = 48
LANES = 128
LEAD = 5.217319695266324
TAIL = (-2.2719599305658895, 2.482104102078497, -1.26081348824302, 0.1916653466086582)


def tile_values(cx, cy, cz, fx, fy, fz):
    dx = cx - fx
    dy = cy - fy
    dz = cz - fz
    sq = dx * dx + dy * dy + dz * dz
    inv = lax.rsqrt(sq)
    turns = sq * inv
    rest = turns - jnp.round(turns)
    z = rest * rest
    p = z + TAIL[0]
    for c in TAIL[1:]:
        p = p * z + c
    return (rest * inv) * p


def high(a):
    return a.astype(jnp.bfloat16).astype(jnp.float32)


def quad_body(nfl, nfirst, *refs):
    center = refs[0]
    fluids = refs[1:1 + nfl]
    n = 1 + nfl
    load_in = refs[n] if nfirst[0] else None
    n += nfirst[0]
    motion_in = refs[n] if nfirst[1] else None
    n += nfirst[1]
    load_out = refs[n]
    motion_outs = refs[n + 1:n + 1 + nfl]
    cpos, cval, fval, fpos, t0, t1, acc, loads = refs[n + 1 + nfl:]
    hf = fluids[0].shape[0]
    nf = nfl * hf
    nb = center.shape[0] // 2
    half = lax.broadcasted_iota(jnp.int32, (1, LANES), 1) < LANES // 2
    for k in range(nf):
        s = slice(k * LANES, (k + 1) * LANES)
        chunk = fluids[k // hf].at[k % hf]
        val = chunk[3:3 + COLS, :] * LEAD
        hi = high(val)
        fval[0:COLS, s] = hi
        fval[COLS:2 * COLS, s] = val - hi
        fpos[:, s] = chunk[0:3, :] * float(WAVES)
    for b in range(nb):
        one = center[2 * b]
        two = center[2 * b + 1]
        top = jnp.where(half, one, pltpu.roll(two, LANES // 2, 1))
        bot = jnp.where(half, pltpu.roll(one, LANES // 2, 1), two)
        val = jnp.concatenate([top[0:24], bot[0:24]], 0) * LEAD
        hi = high(val)
        v = jnp.concatenate([hi, val - hi], 0)
        cval[b, :, 0:LANES] = v
        cval[b, :, LANES:2 * LANES] = v
        pos = jnp.concatenate([top[24:26], bot[24:25], jnp.zeros((5, LANES), jnp.float32)], 0) * float(WAVES)
        post = jnp.transpose(pos)
        for a in range(3):
            cpos[a, b * LANES:(b + 1) * LANES, :] = jnp.broadcast_to(post[:, a:a + 1], (LANES, LANES))

    def compute(b, t):
        for k in range(nf):
            s = slice(k * LANES, (k + 1) * LANES)
            fx = fpos[0:1, s]
            fy = fpos[1:2, s]
            fz = fpos[2:3, s]
            for g in range(LANES // 8):
                rows = slice(b * LANES + g * 8, b * LANES + (g + 1) * 8)
                v = tile_values(cpos[0, rows, :], cpos[1, rows, :], cpos[2, rows, :], fx, fy, fz)
                t[g * 8:(g + 1) * 8, s] = v
                t[LANES + g * 8:LANES + (g + 1) * 8, s] = v - high(v)

    def dots(b, t):
        m = jnp.dot(cval[b], t[...], preferred_element_type=jnp.float32)
        if b == 0:
            acc[...] = m
        else:
            acc[...] += m
        back = lax.dot_general(t[...], fval[...], (((1,), (1,)), ((), ())), preferred_element_type=jnp.float32)
        loads[b * LANES:(b + 1) * LANES, :] = back[0:LANES, :] + back[LANES:2 * LANES, :]

    ts = (t0, t1)
    compute(0, t0)
    for b in range(nb):
        if b + 1 < nb:
            compute(b + 1, ts[(b + 1) % 2])
        dots(b, ts[b % 2])

    for k in range(nf):
        s = slice(k * LANES, (k + 1) * LANES)
        m = acc[0:COLS, s] + acc[COLS:2 * COLS, s]
        if motion_in is not None and k < hf:
            m = m + motion_in[k]
        motion_outs[k // hf][k % hf] = m
    for b in range(nb):
        l = jnp.transpose(loads[b * LANES:(b + 1) * LANES, :])
        l = l[0:COLS] + l[COLS:2 * COLS]
        top = l[0:24]
        bot = l[24:48]
        one = jnp.where(half, top, pltpu.roll(bot, LANES // 2, 1))
        two = jnp.where(half, pltpu.roll(top, LANES // 2, 1), bot)
        if load_in is not None:
            one = one + load_in[2 * b]
            two = two + load_in[2 * b + 1]
        load_out[2 * b] = one
        load_out[2 * b + 1] = two


def quad(center, fluids, load=None, motion=None):
    hf = fluids[0].shape[0]
    hc = center.shape[0]
    nb = hc // 2
    width = len(fluids) * hf * LANES
    extra = tuple(a for a in (load, motion) if a is not None)

    def body(*refs):
        quad_body(len(fluids), (load is not None, motion is not None), *refs)

    vm = pl.BlockSpec(memory_space=pltpu.VMEM)
    return pl.pallas_call(
        body,
        out_shape=(jax.ShapeDtypeStruct((hc, COLS // 2, LANES), jnp.float32),)
        + (jax.ShapeDtypeStruct((hf, COLS, LANES), jnp.float32),) * len(fluids),
        in_specs=[vm] * (1 + len(fluids) + len(extra)),
        out_specs=(vm,) * (1 + len(fluids)),
        scratch_shapes=[
            pltpu.VMEM((3, nb * LANES, LANES), jnp.float32),
            pltpu.VMEM((nb, 2 * COLS, 2 * LANES), jnp.float32),
            pltpu.VMEM((2 * COLS, width), jnp.float32),
            pltpu.VMEM((3, width), jnp.float32),
            pltpu.VMEM((2 * LANES, width), jnp.float32),
            pltpu.VMEM((2 * LANES, width), jnp.float32),
            pltpu.VMEM((2 * COLS, width), jnp.float32),
            pltpu.VMEM((nb * LANES, 2 * COLS), jnp.float32),
        ],
        compiler_params=pltpu.CompilerParams(vmem_limit_bytes=20 * 2**20),
    )(center, *fluids, *extra)


def pack_body(center, out):
    half = center.shape[1]
    out[0:24, 0:half] = center[3:27, :]
    out[0:24, half:] = center[27:51, :]
    out[24:26, 0:half] = center[0:2, :]
    out[24:25, half:] = center[2:3, :]
    out[25:26, half:] = jnp.zeros((1, half), jnp.float32)


def packed(center):
    return pl.pallas_call(
        pack_body,
        out_shape=jax.ShapeDtypeStruct((26, LANES), jnp.float32),
        in_specs=[pl.BlockSpec(memory_space=pltpu.VMEM)],
        out_specs=pl.BlockSpec(memory_space=pltpu.VMEM),
        compiler_params=pltpu.CompilerParams(vmem_limit_bytes=2**20),
        name="pack",
    )(center)


AXES = ("row", "col")


def place(x, y, z, core):
    return (y * 4 + (z // 4) * 2 + core) * 16 + (z % 4) * 4 + x


def partners(move):
    spots = [(x, y, z, c) for x in range(4) for y in range(4) for z in range(8) for c in range(2)]
    return [(place(*spot), place(*move(*spot))) for spot in spots]


def near(v):
    return v ^ 1


def wrap(v):
    return 3 - v


FLUID_STAGES = (
    partners(lambda x, y, z, c: (x, y, z ^ 2, c)),
    partners(lambda x, y, z, c: (near(x), y, z, c)),
    partners(lambda x, y, z, c: (wrap(x), y, z, c)),
    partners(lambda x, y, z, c: (x, y, z, 1 - c)),
)
CENTER_STAGES = (
    partners(lambda x, y, z, c: (x, y, z ^ 1, c)),
    partners(lambda x, y, z, c: (x, y, 2 * wrap(z // 2) + z % 2, c)),
    partners(lambda x, y, z, c: (x, near(y), z, c)),
    partners(lambda x, y, z, c: (x, wrap(y), z, c)),
)


def gather_step(held, stage):
    return held, lax.ppermute(held, AXES, stage)


def sum_step(mine, theirs, stage):
    arrived = lax.ppermute(theirs, AXES, stage)
    half = mine.shape[0] // 2
    return mine[:half] + arrived[:half], mine[half:] + arrived[half:]


def per_device(fluid_data, center_data, poly_coef):
    fluid = fluid_data[None]
    center = packed(center_data)[None]
    fluids = (fluid, None)
    centers = (center, None)
    for i in range(4):
        held = centers[0] if i == 0 else jnp.concatenate(centers, 0)
        centers = gather_step(held, CENTER_STAGES[i])
        held = fluids[0] if i == 0 else jnp.concatenate(fluids, 0)
        fluids = gather_step(held, FLUID_STAGES[i])
    loads, motion = quad(centers[0], fluids[:1])
    loads_away, motion, motion_away = quad(centers[1], fluids, motion=motion)
    loads, motion_away = quad(centers[0], fluids[1:], load=loads, motion=motion_away)
    for i in (3, 2, 1):
        loads, loads_away = sum_step(loads, loads_away, CENTER_STAGES[i])
        motion, motion_away = sum_step(motion, motion_away, FLUID_STAGES[i])
    loads = (loads + lax.ppermute(loads_away, AXES, CENTER_STAGES[0]))[0]
    motion = (motion + lax.ppermute(motion_away, AXES, FLUID_STAGES[0]))[0]
    affine = poly_coef[:, 0:1] + jnp.dot(
        poly_coef[:, 1:],
        fluid_data[:3],
        precision=lax.Precision.HIGHEST,
        preferred_element_type=jnp.float32,
    )
    half = center_data.shape[1]
    return (motion + affine, jnp.concatenate([loads[:, :half], loads[:, half:]], 0))


def solution(mesh):
    placed = (P(None, ("row", "col")), P(None, ("col", "row")), P())
    return jax.shard_map(
        per_device,
        mesh=mesh,
        in_specs=placed,
        out_specs=(P(None, ("row", "col")), P(None, ("col", "row"))),
        check_vma=False,
    )
```

```python
import jax
import jax.numpy as jnp
from jax import lax
from jax.experimental import pallas as pl
from jax.experimental.pallas import tpu as pltpu
from jax.sharding import PartitionSpec as P


WAVES = 64
COLS = 48
LANES = 128
LEAD = 5.217319695266324
TAIL = (-2.2719599305658895, 2.482104102078497, -1.26081348824302, 0.1916653466086582)


def tile_values(cx, cy, cz, fx, fy, fz):
    dx = cx - fx
    dy = cy - fy
    dz = cz - fz
    sq = dx * dx + dy * dy + dz * dz
    inv = lax.rsqrt(sq)
    turns = sq * inv
    rest = turns - jnp.round(turns)
    z = rest * rest
    p = z + TAIL[0]
    for c in TAIL[1:]:
        p = p * z + c
    return (rest * inv) * p


def high(a):
    return a.astype(jnp.bfloat16).astype(jnp.float32)


def quad_body(nfl, nfirst, *refs):
    center = refs[0]
    fluids = refs[1:1 + nfl]
    n = 1 + nfl
    load_in = refs[n] if nfirst[0] else None
    n += nfirst[0]
    motion_in = refs[n] if nfirst[1] else None
    n += nfirst[1]
    load_out = refs[n]
    motion_outs = refs[n + 1:n + 1 + nfl]
    cpos, cval, fval, fpos, t0, t1, acc, loads = refs[n + 1 + nfl:]
    hf = fluids[0].shape[0]
    nf = nfl * hf
    nb = center.shape[0] // 52
    half = lax.broadcasted_iota(jnp.int32, (1, LANES), 1) < LANES // 2
    for k in range(nf):
        s = slice(k * LANES, (k + 1) * LANES)
        chunk = fluids[k // hf].at[k % hf]
        val = chunk[3:3 + COLS, :] * LEAD
        hi = high(val)
        fval[0:COLS, s] = hi
        fval[COLS:2 * COLS, s] = val - hi
        fpos[:, s] = chunk[0:3, :] * float(WAVES)
    for b in range(nb):
        one = center[48 * b:48 * b + 24, :]
        two = center[48 * b + 24:48 * b + 48, :]
        top = jnp.where(half, one, pltpu.roll(two, LANES // 2, 1))
        bot = jnp.where(half, pltpu.roll(one, LANES // 2, 1), two)
        val = jnp.concatenate([top, bot], 0) * LEAD
        hi = high(val)
        v = jnp.concatenate([hi, val - hi], 0)
        cval[b, :, 0:LANES] = v
        cval[b, :, LANES:2 * LANES] = v
        place_one = center[48 * nb + 4 * b:48 * nb + 4 * b + 2, :]
        place_two = center[48 * nb + 4 * b + 2:48 * nb + 4 * b + 4, :]
        top = jnp.where(half, place_one, pltpu.roll(place_two, LANES // 2, 1))
        bot = jnp.where(half, pltpu.roll(place_one, LANES // 2, 1), place_two)
        pos = jnp.concatenate([top, bot[0:1], jnp.zeros((5, LANES), jnp.float32)], 0) * float(WAVES)
        post = jnp.transpose(pos)
        for a in range(3):
            cpos[a, b * LANES:(b + 1) * LANES, :] = jnp.broadcast_to(post[:, a:a + 1], (LANES, LANES))

    def compute(b, t):
        for k in range(nf):
            s = slice(k * LANES, (k + 1) * LANES)
            fx = fpos[0:1, s]
            fy = fpos[1:2, s]
            fz = fpos[2:3, s]
            for g in range(LANES // 8):
                rows = slice(b * LANES + g * 8, b * LANES + (g + 1) * 8)
                v = tile_values(cpos[0, rows, :], cpos[1, rows, :], cpos[2, rows, :], fx, fy, fz)
                t[g * 8:(g + 1) * 8, s] = v
                t[LANES + g * 8:LANES + (g + 1) * 8, s] = v - high(v)

    def dots(b, t):
        m = jnp.dot(cval[b], t[...], preferred_element_type=jnp.float32)
        if b == 0:
            acc[...] = m
        else:
            acc[...] += m
        back = lax.dot_general(t[...], fval[...], (((1,), (1,)), ((), ())), preferred_element_type=jnp.float32)
        loads[b * LANES:(b + 1) * LANES, :] = back[0:LANES, :] + back[LANES:2 * LANES, :]

    ts = (t0, t1)
    compute(0, t0)
    for b in range(nb):
        if b + 1 < nb:
            compute(b + 1, ts[(b + 1) % 2])
        dots(b, ts[b % 2])

    for k in range(nf):
        s = slice(k * LANES, (k + 1) * LANES)
        m = acc[0:COLS, s] + acc[COLS:2 * COLS, s]
        if motion_in is not None and k < hf:
            m = m + motion_in[k]
        motion_outs[k // hf][k % hf] = m
    for b in range(nb):
        l = jnp.transpose(loads[b * LANES:(b + 1) * LANES, :])
        l = l[0:COLS] + l[COLS:2 * COLS]
        top = l[0:24]
        bot = l[24:48]
        one = jnp.where(half, top, pltpu.roll(bot, LANES // 2, 1))
        two = jnp.where(half, pltpu.roll(top, LANES // 2, 1), bot)
        if load_in is not None:
            one = one + load_in[2 * b]
            two = two + load_in[2 * b + 1]
        load_out[2 * b] = one
        load_out[2 * b + 1] = two


def quad(center, fluids, load=None, motion=None):
    hf = fluids[0].shape[0]
    nb = center.shape[0] // 52
    hc = 2 * nb
    width = len(fluids) * hf * LANES
    extra = tuple(a for a in (load, motion) if a is not None)

    def body(*refs):
        quad_body(len(fluids), (load is not None, motion is not None), *refs)

    vm = pl.BlockSpec(memory_space=pltpu.VMEM)
    return pl.pallas_call(
        body,
        out_shape=(jax.ShapeDtypeStruct((hc, COLS // 2, LANES), jnp.float32),)
        + (jax.ShapeDtypeStruct((hf, COLS, LANES), jnp.float32),) * len(fluids),
        in_specs=[vm] * (1 + len(fluids) + len(extra)),
        out_specs=(vm,) * (1 + len(fluids)),
        scratch_shapes=[
            pltpu.VMEM((3, nb * LANES, LANES), jnp.float32),
            pltpu.VMEM((nb, 2 * COLS, 2 * LANES), jnp.float32),
            pltpu.VMEM((2 * COLS, width), jnp.float32),
            pltpu.VMEM((3, width), jnp.float32),
            pltpu.VMEM((2 * LANES, width), jnp.float32),
            pltpu.VMEM((2 * LANES, width), jnp.float32),
            pltpu.VMEM((2 * COLS, width), jnp.float32),
            pltpu.VMEM((nb * LANES, 2 * COLS), jnp.float32),
        ],
        compiler_params=pltpu.CompilerParams(vmem_limit_bytes=20 * 2**20),
    )(center, *fluids, *extra)


def pack_body(center, out):
    half = center.shape[1]
    out[0:24, 0:half] = center[3:27, :]
    out[0:24, half:] = center[27:51, :]
    out[24:26, 0:half] = center[0:2, :]
    out[24:25, half:] = center[2:3, :]
    out[25:26, half:] = jnp.zeros((1, half), jnp.float32)


def packed(center):
    return pl.pallas_call(
        pack_body,
        out_shape=jax.ShapeDtypeStruct((26, LANES), jnp.float32),
        in_specs=[pl.BlockSpec(memory_space=pltpu.VMEM)],
        out_specs=pl.BlockSpec(memory_space=pltpu.VMEM),
        compiler_params=pltpu.CompilerParams(vmem_limit_bytes=2**20),
        name="pack",
    )(center)


AXES = ("row", "col")


def place(x, y, z, core):
    return (y * 4 + (z // 4) * 2 + core) * 16 + (z % 4) * 4 + x


def partners(move):
    spots = [(x, y, z, c) for x in range(4) for y in range(4) for z in range(8) for c in range(2)]
    return [(place(*spot), place(*move(*spot))) for spot in spots]


def near(v):
    return v ^ 1


def wrap(v):
    return 3 - v


def first_hop(v, core):
    return wrap(v) if core else near(v)


def second_hop(v, core):
    return near(v) if core else wrap(v)


FLUID_STAGES = (
    partners(lambda x, y, z, c: (x, y, z ^ 2, c)),
    partners(lambda x, y, z, c: (first_hop(x, c), y, z, c)),
    partners(lambda x, y, z, c: (second_hop(x, c), y, z, c)),
    partners(lambda x, y, z, c: (x, y, z, 1 - c)),
)
CENTER_STAGES = (
    partners(lambda x, y, z, c: (x, y, 2 * wrap(z // 2) + z % 2 if c else z ^ 1, c)),
    partners(lambda x, y, z, c: (x, y, z ^ 1 if c else 2 * wrap(z // 2) + z % 2, c)),
    partners(lambda x, y, z, c: (x, first_hop(y, c), z, c)),
    partners(lambda x, y, z, c: (x, second_hop(y, c), z, c)),
)


def gather_step(held, stage):
    return held, lax.ppermute(held, AXES, stage)


def center_rows(mine, theirs):
    cut = mine.shape[0] // 26 * 24
    return jnp.concatenate([mine[:cut], theirs[:cut], mine[cut:], theirs[cut:]], 0)


def sum_step(mine, theirs, stage):
    arrived = lax.ppermute(theirs, AXES, stage)
    half = mine.shape[0] // 2
    return mine[:half] + arrived[:half], mine[half:] + arrived[half:]


def per_device(fluid_data, center_data, poly_coef):
    fluid = fluid_data[None]
    center = packed(center_data)
    fluids = (fluid, None)
    centers = (center, None)
    for i in range(4):
        held = centers[0] if i == 0 else center_rows(*centers)
        centers = gather_step(held, CENTER_STAGES[i])
        held = fluids[0] if i == 0 else jnp.concatenate(fluids, 0)
        fluids = gather_step(held, FLUID_STAGES[i])
    loads, motion = quad(centers[0], fluids[:1])
    loads_away, motion, motion_away = quad(centers[1], fluids, motion=motion)
    loads, motion_away = quad(centers[0], fluids[1:], load=loads, motion=motion_away)
    for i in (3, 2, 1):
        loads, loads_away = sum_step(loads, loads_away, CENTER_STAGES[i])
        motion, motion_away = sum_step(motion, motion_away, FLUID_STAGES[i])
    loads = (loads + lax.ppermute(loads_away, AXES, CENTER_STAGES[0]))[0]
    motion = (motion + lax.ppermute(motion_away, AXES, FLUID_STAGES[0]))[0]
    affine = poly_coef[:, 0:1] + jnp.dot(
        poly_coef[:, 1:],
        fluid_data[:3],
        precision=lax.Precision.HIGHEST,
        preferred_element_type=jnp.float32,
    )
    half = center_data.shape[1]
    return (motion + affine, jnp.concatenate([loads[:, :half], loads[:, half:]], 0))


def solution(mesh):
    placed = (P(None, ("row", "col")), P(None, ("col", "row")), P())
    return jax.shard_map(
        per_device,
        mesh=mesh,
        in_specs=placed,
        out_specs=(P(None, ("row", "col")), P(None, ("col", "row"))),
        check_vma=False,
    )
```
